32 devices in a mesh: layer: 4 (over x, core), harm: 8 (over z, y).
Axes of the slice: x: 2, y: 2, z: 4, core: 2. Of those that a mesh axis runs over, the one named last changes fastest.
Arguments:
- source: bfloat16 [2, 2048, 128], P(None, 'harm'), may hold values from -6 to 6
- transfer: bfloat16 [4, 2, 2048, 2048], P('layer', None, 'harm'), may hold values from -0.09375 to 0.09375
- fields: bfloat16 [4, 2, 2048, 128], P('layer', None, 'harm'), may hold values from -6 to 6
- orders: int32 [2048], replicated, may hold values from 0 to 2047, each once
Outputs:
- gradients: float32 [4, 2, 4096], P('layer', None, 'harm')
- boundary: bfloat16 [4, 2, 2048, 128], P('layer', None, 'harm')
The draws below stay inside these ranges and needn't reach their ends.
Inputs may be any that keep to these rules, and one draw needn't show every extreme that they name: `orders`: every value from 0 to 2047 appears exactly once.
All inputs are finite; a program needn't handle non-finite values.
Results may differ from the reference program's by a relative error of at most 0.006.
Values may be sent and summed in bfloat16 or wider, within the bound.
A program may use at most 64 MiB of HBM per device.

```python
import math
import jax
import jax.numpy as jnp
from jax import lax

HARM = 2048
LAYERS_DEV = 1
BATCH = 128
LAYERS = 4
N_HARM = 8


def shard_levels(key, extent, shards, least, high):
    def one(dim, blocks):
        draws = jax.random.uniform(jax.random.fold_in(jax.random.fold_in(key, 6), dim), (blocks,), jnp.float32, least / len(shards), high / len(shards))
        return jnp.repeat(jnp.exp(draws), extent[dim] // blocks).reshape((-1,) + (1,) * (len(extent) - dim - 1))

    level = one(*shards[0])
    for cut in shards[1:]:
        level = level * one(*cut)
    return level


def normal_values(stream_key, shape, deviation, bound, cuts=(), kind=jnp.bfloat16):
    drawn = jax.random.normal(stream_key, shape, jnp.float32) * deviation
    if len(cuts) > 0:
        drawn = shard_levels(stream_key, shape, cuts, -0.22, 0.18) * drawn
    return jnp.clip(drawn, min=-bound, max=bound).astype(kind)


def setup_inputs(seed: int = 0) -> dict:
    splits = jax.random.split(jax.random.key(seed), 5)
    source = normal_values(splits[0], (2, HARM, BATCH), 1.0, 6.0, ((1, 8),))
    transfer = normal_values(splits[1], (LAYERS, 2, HARM, HARM), (2 * HARM) ** -0.5, 0.09375, ((0, 4), (2, 8)))
    fields = normal_values(splits[2], (LAYERS, 2, HARM, BATCH), 1.0, 6.0, ((0, 4), (2, 8)))
    orders = jax.random.permutation(splits[3], HARM).astype(jnp.int32)
    return dict(source=source, transfer=transfer, fields=fields, orders=orders)


def correlate(adjoint, forward, position, band_start, band_width):
    harmonics = adjoint.shape[1]
    columns = adjoint.shape[2]
    adj_sorted = jnp.take(adjoint, position, axis=1).astype(jnp.float32)
    fwd_sorted = jnp.take(forward, position, axis=1).astype(jnp.float32)
    padded = jnp.pad(adj_sorted, ((0, 0), (harmonics, harmonics + 1), (0, 0)))
    window_slab = lax.dynamic_slice_in_dim(padded, band_start + 1, harmonics + band_width, 1)
    count = harmonics // band_width
    blocks = window_slab.reshape(2, count + 1, band_width, columns)
    windows = jnp.concatenate([blocks[:, :-1], blocks[:, 1:]], axis=2)
    forward_blocks = fwd_sorted.reshape(2, count, band_width, columns)

    def product(left_part, right_part):
        return jnp.einsum('nkb,ncb->nkc', left_part, right_part)
    real_part = product(forward_blocks[0], windows[0]) - product(forward_blocks[1], windows[1])
    imag_part = product(forward_blocks[0], windows[1]) + product(forward_blocks[1], windows[0])

    def diagonals(result_block):
        flattened = result_block.reshape(count, band_width * 2 * band_width)
        flattened = jnp.pad(flattened, ((0, 0), (0, band_width)))
        shaped = flattened.reshape(count, band_width, 2 * band_width + 1)[:, :, :band_width]
        return lax.optimization_barrier(jnp.sum(shaped, axis=(0, 1)))
    return jnp.stack([diagonals(real_part), diagonals(imag_part)])

def reference(source, transfer, fields, orders):
    harmonics = orders.shape[0]
    columns = source.shape[2]
    layer_count = transfer.shape[0]
    position = jnp.zeros((harmonics,), jnp.int32).at[orders].set(jnp.arange(harmonics, dtype=jnp.int32))
    band_width = 2 * harmonics // N_HARM
    norm_scale = 1.0 / math.sqrt(harmonics * columns)
    starts = jnp.arange(0, 2 * harmonics, band_width, dtype=jnp.int32)
    adjoint = source
    grads = [None] * layer_count
    bounds = []
    for layer_index in range(layer_count - 1, -1, -1):
        forward = fields[layer_index]
        bands = lax.map(lambda band_start: correlate(adjoint, forward, position, band_start, band_width), starts)
        grads[layer_index] = jnp.transpose(bands, (1, 0, 2)).reshape(2, 2 * harmonics) * norm_scale
        matrix = transfer[layer_index]
        real_part = jnp.dot(matrix[0], adjoint[0], preferred_element_type=jnp.float32) - jnp.dot(matrix[1], adjoint[1], preferred_element_type=jnp.float32)
        imag_part = jnp.dot(matrix[0], adjoint[1], preferred_element_type=jnp.float32) + jnp.dot(matrix[1], adjoint[0], preferred_element_type=jnp.float32)
        adjoint = jnp.stack([real_part, imag_part]).astype(jnp.bfloat16)
        if layer_index % LAYERS_DEV == 0:
            bounds.append(adjoint)
    return (jnp.stack(grads), jnp.stack(bounds[::-1]))
```

```python
import functools
import math

import jax
import jax.numpy as jnp
from jax import lax
from jax.experimental import pallas as pl
from jax.experimental.pallas import tpu as pltpu
from jax.sharding import PartitionSpec as P

MESH = pl.DeviceIdType.MESH


def flipped(index, bits, count):
    total = 0
    place = 1
    while place < count:
        digit = (index // place) % 2
        total = total + (1 - digit if (bits // place) % 2 else digit) * place
        place *= 2
    return total


def sweep_kernel(
    sections,
    members,
    inner,
    block,
    source_ref,
    transfer_ref,
    fields_ref,
    orders_ref,
    grads_ref,
    bottom_ref,
    matrix,
    adj,
    fwd,
    out_block,
    onehot,
    left,
    padded,
    local_sems,
    adj_recv,
    fwd_recv,
    adj_send,
    adj_forward,
    down_send,
    fwd_send,
    fwd_forward,
):
    outer = members // inner
    section = lax.axis_index("layer")
    member = lax.axis_index("harm")
    o_index, i_index = member // inner, member % inner
    rows = out_block.shape[0]
    harmonics = adj.shape[0]
    columns = adj.shape[1] // 2
    band = 2 * harmonics // members
    width = block + band
    top = section == sections - 1
    early = section < sections // 2

    def rows_of(index):
        return pl.ds(pl.multiple_of(index * rows, rows), rows)

    load_matrix = pltpu.make_async_copy(transfer_ref.at[0], matrix, local_sems.at[0])
    load_matrix.start()
    loads = []
    for part in range(2):
        lanes = pl.ds(part * columns, columns)
        loads.append(
            pltpu.make_async_copy(fields_ref.at[0, part], fwd.at[rows_of(member), lanes], local_sems.at[1 + part])
        )
        loads.append(
            pltpu.make_async_copy(source_ref.at[part], adj.at[rows_of(member), lanes], local_sems.at[3 + part])
        )
    loads[0].start()
    loads[2].start()

    @pl.when(top)
    def _():
        loads[1].start()
        loads[3].start()

    barrier = pltpu.get_barrier_semaphore()
    peers = [(section, flipped(o_index, t, outer) * inner + i_index) for t in range(1, outer)]
    peers += [(section, o_index * inner + flipped(i_index, u, inner)) for u in range(1, inner)]
    for step in (1, sections - 1):
        peers += [((section + step) % sections, flipped(o_index, t, outer) * inner + i_index) for t in range(outer)]
    for peer in peers:
        pl.semaphore_signal(barrier, inc=1, device_id=peer, device_id_type=MESH)
    padded[: harmonics, :] = jnp.zeros((harmonics, 2 * columns), padded.dtype)
    padded[2 * harmonics :, :] = jnp.zeros((harmonics, 2 * columns), padded.dtype)
    loads[0].wait()
    loads[2].wait()

    @pl.when(top)
    def _():
        loads[1].wait()
        loads[3].wait()

    pl.semaphore_wait(barrier, len(peers))

    def line_copy(buffer, send, recv, t):
        target = flipped(o_index, t, outer) * inner + i_index
        return pltpu.make_async_remote_copy(
            src_ref=buffer.at[rows_of(member)],
            dst_ref=buffer.at[rows_of(member)],
            send_sem=send.at[t],
            recv_sem=recv.at[member],
            device_id=(section, target),
            device_id_type=MESH,
        )

    def down_copy(t):
        target = flipped(o_index, t, outer) * inner + i_index
        return pltpu.make_async_remote_copy(
            src_ref=out_block,
            dst_ref=adj.at[rows_of(member)],
            send_sem=down_send.at[t],
            recv_sem=adj_recv.at[member],
            device_id=(section - 1, target),
            device_id_type=MESH,
        )

    def forward_copy(buffer, send, recv, t, u):
        held = flipped(o_index, t, outer) * inner + i_index
        target = o_index * inner + flipped(i_index, u, inner)
        return pltpu.make_async_remote_copy(
            src_ref=buffer.at[rows_of(held)],
            dst_ref=buffer.at[rows_of(held)],
            send_sem=send.at[t, u],
            recv_sem=recv.at[held],
            device_id=(section, target),
            device_id_type=MESH,
        )

    def arrival(buffer, recv, index):
        return pltpu.make_async_remote_copy(
            src_ref=buffer.at[rows_of(index)],
            dst_ref=buffer.at[rows_of(index)],
            send_sem=recv.at[index],
            recv_sem=recv.at[index],
            device_id=(section, index),
            device_id_type=MESH,
        )

    def start_line(buffer, send, recv):
        for t in range(1, outer):
            line_copy(buffer, send, recv, t).start()

    def relay(buffer, recv, forward, t):
        for u in range(1, inner):
            forward_copy(buffer, forward, recv, t, u).start()

    def collect(buffer, recv, forward, own_here):
        for t in range(outer):
            held = flipped(o_index, t, outer) * inner + i_index
            if t == 0 and own_here is True:
                pass
            elif t == 0 and own_here is not False:

                @pl.when(jnp.logical_not(own_here))
                def _():
                    arrival(buffer, recv, held).wait_recv()
            else:
                arrival(buffer, recv, held).wait_recv()
            relay(buffer, recv, forward, t)
        for t in range(outer):
            for u in range(1, inner):
                held = flipped(o_index, t, outer) * inner + flipped(i_index, u, inner)
                arrival(buffer, recv, held).wait_recv()

    def finish_forwards(buffer, recv, forward):
        for t in range(outer):
            for u in range(1, inner):
                forward_copy(buffer, forward, recv, t, u).wait_send()

    def finish_line(buffer, send, recv):
        for t in range(1, outer):
            line_copy(buffer, send, recv, t).wait_send()

    def gather_fields():
        start_line(fwd, fwd_send, fwd_recv)
        collect(fwd, fwd_recv, fwd_forward, True)

    def build_onehot(reverse):
        tile = block

        @pl.loop(0, harmonics // tile)
        def _(index):
            start = pl.multiple_of(index * tile, tile)
            line = lax.broadcasted_iota(jnp.int32, (tile, harmonics), 0)
            wanted = start + (tile - 1 - line if reverse else line)
            onehot[pl.ds(start, tile), :] = jnp.where(orders_ref[...] == wanted, 1.0, 0.0).astype(onehot.dtype)

    def sort_fields():
        build_onehot(True)

        @pl.loop(0, harmonics // block)
        def _(index):
            start = pl.multiple_of(index * block, block)
            sorted_rows = jnp.dot(onehot[pl.ds(start, block), :], fwd[...], preferred_element_type=jnp.float32)
            real, imag = sorted_rows[:, :columns], sorted_rows[:, columns:]
            left[index, :block, :] = jnp.concatenate([real, -imag], axis=1).astype(left.dtype)
            left[index, block:, :] = jnp.concatenate([imag, real], axis=1).astype(left.dtype)

        build_onehot(False)

    @pl.when(early)
    def _():
        gather_fields()
        sort_fields()

    @pl.when(top)
    def _():
        start_line(adj, adj_send, adj_recv)

    load_matrix.wait()
    collect(adj, adj_recv, adj_forward, top)

    by_real = jnp.dot(matrix[0], adj[...], preferred_element_type=jnp.float32)
    by_imag = jnp.dot(matrix[1], adj[...], preferred_element_type=jnp.float32)
    result = jnp.concatenate(
        [by_real[:, :columns] - by_imag[:, columns:], by_real[:, columns:] + by_imag[:, :columns]], axis=1
    ).astype(out_block.dtype)
    out_block[...] = result
    bottom_ref[...] = result

    @pl.when(section > 0)
    def _():
        for t in range(outer):
            down_copy(t).start()

    @pl.when(jnp.logical_not(early))
    def _():
        gather_fields()
        sort_fields()

    tile = 2 * block if harmonics % (2 * block) == 0 else block

    @pl.loop(0, harmonics // tile)
    def _(index):
        start = pl.multiple_of(index * tile, tile)
        padded[pl.ds(pl.multiple_of(harmonics + start, tile), tile), :] = jnp.dot(
            onehot[pl.ds(start, tile), :], adj[...], preferred_element_type=jnp.float32
        ).astype(padded.dtype)

    total = jnp.zeros((2 * block, width), jnp.float32)
    for index in range(harmonics // block):
        window = padded[pl.ds(pl.multiple_of(member * band + index * block, block), width), :]
        total = total + lax.dot_general(
            left[index], window, (((1,), (1,)), ((), ())), preferred_element_type=jnp.float32
        )
    for part in range(2):
        rolled = pltpu.roll(
            total[part * block : (part + 1) * block], width - block, 1, stride=1, stride_axis=0
        )
        grads_ref[part : part + 1, :] = jnp.sum(rolled, axis=0, keepdims=True)[:, :band]

    finish_forwards(adj, adj_recv, adj_forward)
    finish_line(fwd, fwd_send, fwd_recv)
    finish_forwards(fwd, fwd_recv, fwd_forward)

    @pl.when(top)
    def _():
        finish_line(adj, adj_send, adj_recv)

    @pl.when(section > 0)
    def _():
        for t in range(outer):
            down_copy(t).wait_send()


def per_device(source, transfer, fields, orders):
    harmonics = orders.shape[0]
    sections = lax.axis_size("layer")
    members = lax.axis_size("harm")
    rows = transfer.shape[2]
    columns = source.shape[2]
    inner = 1 << ((members.bit_length() - 1) // 2)
    outer = members // inner
    band = 2 * harmonics // members
    block = min(128, band)
    norm_scale = 1.0 / math.sqrt(harmonics * columns)
    any_space = pl.BlockSpec(memory_space=pl.ANY)
    vmem = pl.BlockSpec(memory_space=pltpu.VMEM)
    dma = pltpu.SemaphoreType.DMA
    grads, bottom = pl.pallas_call(
        functools.partial(sweep_kernel, sections, members, inner, block),
        out_shape=(
            jax.ShapeDtypeStruct((2, band), jnp.float32),
            jax.ShapeDtypeStruct((rows, 2 * columns), jnp.bfloat16),
        ),
        in_specs=[any_space, any_space, any_space, vmem],
        out_specs=(vmem, vmem),
        scratch_shapes=[
            pltpu.VMEM((2, rows, harmonics), jnp.bfloat16),
            pltpu.VMEM((harmonics, 2 * columns), jnp.bfloat16),
            pltpu.VMEM((harmonics, 2 * columns), jnp.bfloat16),
            pltpu.VMEM((rows, 2 * columns), jnp.bfloat16),
            pltpu.VMEM((harmonics, harmonics), jnp.bfloat16),
            pltpu.VMEM((harmonics // block, 2 * block, 2 * columns), jnp.bfloat16),
            pltpu.VMEM((3 * harmonics, 2 * columns), jnp.bfloat16),
            dma((5,)),
            dma((members,)),
            dma((members,)),
            dma((outer,)),
            dma((outer, inner)),
            dma((outer,)),
            dma((outer,)),
            dma((outer, inner)),
        ],
        compiler_params=pltpu.CompilerParams(collective_id=0, has_side_effects=True),
        name="sweep",
    )(source, transfer, fields, orders.reshape(1, harmonics))
    boundary = jnp.stack([bottom[:, :columns], bottom[:, columns:]])[None]
    return (grads * norm_scale)[None], boundary


def solution(mesh):
    return jax.shard_map(
        per_device,
        mesh=mesh,
        in_specs=(
            P(None, "harm", None),
            P("layer", None, "harm", None),
            P("layer", None, "harm", None),
            P(),
        ),
        out_specs=(P("layer", None, "harm"), P("layer", None, "harm", None)),
        check_vma=False,
    )
```

```python
import functools
import math

import jax
import jax.numpy as jnp
from jax import lax
from jax.experimental import pallas as pl
from jax.experimental.pallas import tpu as pltpu
from jax.sharding import PartitionSpec as P

MESH = pl.DeviceIdType.MESH
REACH = 3
CROSS = (0,)
FAR_FIRST = False


def flipped(index, bits, count):
    total = 0
    place = 1
    while place < count:
        digit = (index // place) % 2
        total = total + (1 - digit if (bits // place) % 2 else digit) * place
        place *= 2
    return total


def guarded(condition, action):
    if condition is None:
        action()
    else:
        pl.when(condition)(action)


def sweep_kernel(
    sections,
    members,
    inner,
    block,
    source_ref,
    transfer_ref,
    fields_ref,
    orders_ref,
    grads_ref,
    bottom_ref,
    matrix,
    staged,
    adj,
    fwd,
    out_block,
    onehot_adj,
    onehot_fwd,
    left,
    padded,
    local_sems,
    go_sem,
    adj_recv,
    adj_send,
    adj_relay,
    adj_forward,
    down_send,
    fwd_recv,
    fwd_send,
    fwd_relay,
    fwd_forward,
):
    outer = members // inner
    section = lax.axis_index("layer")
    member = lax.axis_index("harm")
    o_index, i_index = member // inner, member % inner
    rows = out_block.shape[0]
    harmonics = adj.shape[0]
    columns = adj.shape[1] // 2
    chunks = adj_recv.shape[0]
    lanes = adj.shape[1] // chunks
    half = lanes // 2
    band = 2 * harmonics // members
    width = block + band
    top = section == sections - 1
    early = section < sections // 2
    reach = min(REACH, outer - 1)
    near = sorted(range(1 - outer, outer), key=abs)
    order = sorted(range(-reach, reach + 1), key=abs, reverse=FAR_FIRST)

    def rows_of(index):
        return pl.ds(pl.multiple_of(index * rows, rows), rows)

    load_matrix = pltpu.make_async_copy(transfer_ref.at[0], matrix, local_sems.at[0])
    load_source = pltpu.make_async_copy(source_ref, staged, local_sems.at[1])
    load_fields = [
        pltpu.make_async_copy(
            fields_ref.at[0, part], fwd.at[rows_of(member), pl.ds(part * columns, columns)], local_sems.at[2 + part]
        )
        for part in range(2)
    ]
    load_source.start()
    load_matrix.start()
    for load in load_fields:
        load.start()

    barrier = pltpu.get_barrier_semaphore()
    peers = [(section, flipped(member, t, members)) for t in range(1, members)]
    for step in (1, sections - 1):
        peers += [((section + step) % sections, flipped(member, t, members)) for t in range(members)]
    for peer in peers:
        pl.semaphore_signal(barrier, inc=1, device_id=peer, device_id_type=MESH)
    load_source.wait()

    @pl.when(top)
    def _():
        for m in range(chunks):
            span = slice(m * half, (m + 1) * half)
            adj[rows_of(member), m * lanes : (m + 1) * lanes] = jnp.concatenate(
                [staged[0][:, span], staged[1][:, span]], axis=1
            )

    pl.semaphore_wait(barrier, len(peers))

    def present(d):
        return None if d == 0 else jnp.logical_and(o_index + d >= 0, o_index + d < outer)

    def lanes_of(buffer, recv, m):
        size = buffer.shape[1] // recv.shape[0]
        return pl.ds(m * size, size)

    def line_copy(buffer, send, recv, m, d, u, own_section=True):
        span = lanes_of(buffer, recv, m)
        return pltpu.make_async_remote_copy(
            src_ref=buffer.at[rows_of(member), span] if own_section else out_block.at[:, span],
            dst_ref=buffer.at[rows_of(member), span],
            send_sem=send.at[m, d + reach, u],
            recv_sem=recv.at[m, member],
            device_id=(section if own_section else section - 1, (o_index + d) * inner + flipped(i_index, u, inner)),
            device_id_type=MESH,
        )

    def forward_copy(buffer, send, recv, m, d, u):
        span = lanes_of(buffer, recv, m)
        held = member - d * inner
        return pltpu.make_async_remote_copy(
            src_ref=buffer.at[rows_of(held), span],
            dst_ref=buffer.at[rows_of(held), span],
            send_sem=send.at[m, d + outer - 1, u],
            recv_sem=recv.at[m, held],
            device_id=(section, o_index * inner + flipped(i_index, u, inner)),
            device_id_type=MESH,
        )

    def relay_copy(buffer, send, recv, m, d):
        span = lanes_of(buffer, recv, m)
        held = member - d * inner
        return pltpu.make_async_remote_copy(
            src_ref=buffer.at[rows_of(held), span],
            dst_ref=buffer.at[rows_of(held), span],
            send_sem=send.at[m, d + outer - 1],
            recv_sem=recv.at[m, held],
            device_id=(section, member + (inner if d > 0 else -inner)),
            device_id_type=MESH,
        )

    def relays(d):
        return reach <= abs(d) < outer - 1

    def onward(d):
        step = 1 if d > 0 else -1
        return jnp.logical_and(o_index + step >= 0, o_index + step < outer)

    def arrival(buffer, recv, m, index):
        span = lanes_of(buffer, recv, m)
        return pltpu.make_async_remote_copy(
            src_ref=buffer.at[rows_of(index), span],
            dst_ref=buffer.at[rows_of(index), span],
            send_sem=recv.at[m, index],
            recv_sem=recv.at[m, index],
            device_id=(section, index),
            device_id_type=MESH,
        )

    def each_line(buffer, send, recv, m, finish=False, own_section=True):
        for d in order:
            for u in range(inner if abs(d) in CROSS else 1):
                if own_section and d == 0 and u == 0:
                    continue
                copy = line_copy(buffer, send, recv, m, d, u, own_section)
                guarded(present(d), copy.wait_send if finish else copy.start)

    def each_down(m, finish=False):
        each_line(adj, down_send, adj_recv, m, finish, own_section=False)

    def pass_on(buffer, recv, relay, forward, m, d, finish=False):
        if relays(d):
            copy = relay_copy(buffer, relay, recv, m, d)
            guarded(onward(d), copy.wait_send if finish else copy.start)
        for u in range(1, inner if abs(d) not in CROSS else 1):
            copy = forward_copy(buffer, forward, recv, m, d, u)
            if finish:
                copy.wait_send()
            else:
                copy.start()

    def collect_line(buffer, recv, relay, forward, m, own_here):
        for d in near:

            def step(d=d):
                if d == 0 and own_here is None:
                    pass
                elif d == 0:
                    pl.when(jnp.logical_not(own_here))(arrival(buffer, recv, m, member).wait_recv)
                else:
                    arrival(buffer, recv, m, member - d * inner).wait_recv()
                pass_on(buffer, recv, relay, forward, m, d)

            guarded(present(-d), step)

    def collect_inner(buffer, recv, m):
        for t in range(outer):
            for u in range(1, inner):
                held = flipped(o_index, t, outer) * inner + flipped(i_index, u, inner)
                arrival(buffer, recv, m, held).wait_recv()

    def finish_passing(buffer, recv, relay, forward, m):
        for d in near:
            guarded(present(-d), functools.partial(pass_on, buffer, recv, relay, forward, m, d, finish=True))

    def start_fields():
        for m in range(fwd_recv.shape[0]):
            each_line(fwd, fwd_send, fwd_recv, m)

    def relay_fields():
        for m in range(fwd_recv.shape[0]):
            collect_line(fwd, fwd_recv, fwd_relay, fwd_forward, m, None)

    def finish_fields():
        for m in range(fwd_recv.shape[0]):
            collect_inner(fwd, fwd_recv, m)

    def build_onehots():
        @pl.loop(0, harmonics // block)
        def _(index):
            start = pl.multiple_of(index * block, block)
            line = lax.broadcasted_iota(jnp.int32, (block, harmonics), 0)
            orders = orders_ref[...].reshape(1, harmonics) - start
            dtype = onehot_adj.dtype
            onehot_adj[pl.ds(start, block), :] = jnp.where(orders == line, 1.0, 0.0).astype(dtype)
            onehot_fwd[pl.ds(start, block), :] = jnp.where(orders == block - 1 - line, 1.0, 0.0).astype(dtype)

        padded[:harmonics, :] = jnp.zeros((harmonics, 2 * columns), padded.dtype)
        padded[2 * harmonics :, :] = jnp.zeros((harmonics, 2 * columns), padded.dtype)

    def sort_fields():
        @pl.loop(0, harmonics // block)
        def _(index):
            start = pl.multiple_of(index * block, block)
            sorted_rows = jnp.dot(onehot_fwd[pl.ds(start, block), :], fwd[...], preferred_element_type=jnp.float32)
            real, imag = sorted_rows[:, :columns], sorted_rows[:, columns:]
            for_real, for_imag = [], []
            for m in range(chunks):
                span = slice(m * half, (m + 1) * half)
                for_real += [real[:, span], -imag[:, span]]
                for_imag += [imag[:, span], real[:, span]]
            left[index, :block, :] = jnp.concatenate(for_real, axis=1).astype(left.dtype)
            left[index, block:, :] = jnp.concatenate(for_imag, axis=1).astype(left.dtype)

    tile = 2 * block if harmonics % (2 * block) == 0 else block

    def sort_adjoint():
        @pl.loop(0, harmonics // tile)
        def _(index):
            start = pl.multiple_of(index * tile, tile)
            padded[pl.ds(pl.multiple_of(harmonics + start, tile), tile), :] = jnp.dot(
                onehot_adj[pl.ds(start, tile), :], adj[...], preferred_element_type=jnp.float32
            ).astype(padded.dtype)

    @pl.when(top)
    def _():
        for m in range(chunks):
            each_line(adj, adj_send, adj_recv, m)

    for load in load_fields:
        load.wait()

    @pl.when(jnp.logical_not(early) & jnp.logical_not(top))
    def _():
        build_onehots()

    @pl.when(section < sections // 2 - 1)
    def _():
        build_onehots()
        pl.semaphore_wait(go_sem, 1)

    @pl.when(early)
    def _():
        start_fields()

    @pl.when(section == sections // 2 - 1)
    def _():
        build_onehots()

    @pl.when(early)
    def _():
        relay_fields()
        finish_fields()

    @pl.when(early & (section > 0))
    def _():
        pl.semaphore_signal(go_sem, inc=1, device_id=(section - 1, member), device_id_type=MESH)

    @pl.when(early)
    def _():
        sort_fields()

    load_matrix.wait()
    for m in range(chunks):
        collect_line(adj, adj_recv, adj_relay, adj_forward, m, top)
    results = []
    for m in range(chunks):
        collect_inner(adj, adj_recv, m)
        values = adj[:, m * lanes : (m + 1) * lanes]
        by_real = jnp.dot(matrix[0], values, preferred_element_type=jnp.float32)
        by_imag = jnp.dot(matrix[1], values, preferred_element_type=jnp.float32)
        real = by_real[:, :half] - by_imag[:, half:]
        imag = by_real[:, half:] + by_imag[:, :half]
        out_block[:, m * lanes : (m + 1) * lanes] = jnp.concatenate([real, imag], axis=1).astype(out_block.dtype)

        @pl.when(section > 0)
        def _(m=m):
            each_down(m)

    for part in range(2):
        pieces = [out_block[:, m * lanes + part * half : m * lanes + (part + 1) * half] for m in range(chunks)]
        bottom_ref[part] = jnp.concatenate(pieces, axis=1)

    @pl.when(jnp.logical_and(jnp.logical_not(early), jnp.logical_not(top)))
    def _():
        pl.semaphore_signal(go_sem, inc=1, device_id=(section + 1, member), device_id_type=MESH)

    @pl.when(top)
    def _():
        build_onehots()

    @pl.when(section > sections // 2)
    def _():
        pl.semaphore_wait(go_sem, 1)

    @pl.when(jnp.logical_not(early))
    def _():
        start_fields()
        relay_fields()
        sort_adjoint()
        finish_fields()
        sort_fields()

    @pl.when(early)
    def _():
        sort_adjoint()

    total = jnp.zeros((2 * block, width), jnp.float32)
    for index in range(harmonics // block):
        window = padded[pl.ds(pl.multiple_of(member * band + index * block, block), width), :]
        total = total + lax.dot_general(
            left[index], window, (((1,), (1,)), ((), ())), preferred_element_type=jnp.float32
        )
    for part in range(2):
        rolled = pltpu.roll(
            total[part * block : (part + 1) * block], width - block, 1, stride=1, stride_axis=0
        )
        grads_ref[part : part + 1, :] = jnp.sum(rolled, axis=0, keepdims=True)[:, :band]

    for m in range(chunks):
        finish_passing(adj, adj_recv, adj_relay, adj_forward, m)
    for m in range(fwd_recv.shape[0]):
        each_line(fwd, fwd_send, fwd_recv, m, finish=True)
        finish_passing(fwd, fwd_recv, fwd_relay, fwd_forward, m)

    @pl.when(top)
    def _():
        for m in range(chunks):
            each_line(adj, adj_send, adj_recv, m, finish=True)

    @pl.when(section > 0)
    def _():
        for m in range(chunks):
            each_down(m, finish=True)


def per_device(source, transfer, fields, orders):
    harmonics = orders.shape[0]
    sections = lax.axis_size("layer")
    members = lax.axis_size("harm")
    rows = transfer.shape[2]
    columns = source.shape[2]
    inner = 1 << ((members.bit_length() - 1) // 2)
    outer = members // inner
    band = 2 * harmonics // members
    block = min(128, band)
    chunks = max(1, 2 * columns // 128)
    reach = min(REACH, outer - 1)
    norm_scale = 1.0 / math.sqrt(harmonics * columns)
    any_space = pl.BlockSpec(memory_space=pl.ANY)
    vmem = pl.BlockSpec(memory_space=pltpu.VMEM)
    dma = pltpu.SemaphoreType.DMA
    grads, bottom = pl.pallas_call(
        functools.partial(sweep_kernel, sections, members, inner, block),
        out_shape=(
            jax.ShapeDtypeStruct((2, band), jnp.float32),
            jax.ShapeDtypeStruct((2, rows, columns), jnp.bfloat16),
        ),
        in_specs=[any_space, any_space, any_space, vmem],
        out_specs=(vmem, vmem),
        scratch_shapes=[
            pltpu.VMEM((2, rows, harmonics), jnp.bfloat16),
            pltpu.VMEM((2, rows, columns), jnp.bfloat16),
            pltpu.VMEM((harmonics, 2 * columns), jnp.bfloat16),
            pltpu.VMEM((harmonics, 2 * columns), jnp.bfloat16),
            pltpu.VMEM((rows, 2 * columns), jnp.bfloat16),
            pltpu.VMEM((harmonics, harmonics), jnp.bfloat16),
            pltpu.VMEM((harmonics, harmonics), jnp.bfloat16),
            pltpu.VMEM((harmonics // block, 2 * block, 2 * columns), jnp.bfloat16),
            pltpu.VMEM((3 * harmonics, 2 * columns), jnp.bfloat16),
            dma((4,)),
            pltpu.SemaphoreType.REGULAR,
            dma((chunks, members)),
            dma((chunks, 2 * reach + 1, inner)),
            dma((chunks, 2 * outer - 1)),
            dma((chunks, 2 * outer - 1, inner)),
            dma((chunks, 2 * reach + 1, inner)),
            dma((1, members)),
            dma((1, 2 * reach + 1, inner)),
            dma((1, 2 * outer - 1)),
            dma((1, 2 * outer - 1, inner)),
        ],
        compiler_params=pltpu.CompilerParams(collective_id=0, has_side_effects=True),
        name="sweep",
    )(source, transfer, fields, orders)
    return (grads * norm_scale)[None], bottom[None]


def solution(mesh):
    return jax.shard_map(
        per_device,
        mesh=mesh,
        in_specs=(
            P(None, "harm", None),
            P("layer", None, "harm", None),
            P("layer", None, "harm", None),
            P(),
        ),
        out_specs=(P("layer", None, "harm"), P("layer", None, "harm", None)),
        check_vma=False,
    )
```
